128 devices in a mesh: rep: 2 (over core), dp: 64 (over x, y, z).
Axes of the slice: x: 4, y: 4, z: 4, core: 2. Of those that a mesh axis runs over, the one named last changes fastest.
Arguments:
- x: bfloat16 [128, 2048, 1024], P(('rep', 'dp')), parts along dimension 0
- dy: bfloat16 [128, 2048, 1024], P(('rep', 'dp')), parts along dimension 0
- w_gate: bfloat16 [2, 1024, 3200], replicated
- w_up: bfloat16 [2, 1024, 3200], replicated
- w_down: bfloat16 [2, 3200, 1024], replicated
- m_w_gate: float32 [2, 1024, 3200], replicated
- m_w_up: float32 [2, 1024, 3200], replicated
- m_w_down: float32 [2, 3200, 1024], replicated
- v_w_gate: float32 [2, 1024, 3200], replicated
- v_w_up: float32 [2, 1024, 3200], replicated
- v_w_down: float32 [2, 3200, 1024], replicated
Outputs:
- output 1: bfloat16 [4, 1024, 3200], P('rep'), parts along dimension 0
- output 2: bfloat16 [4, 1024, 3200], P('rep'), parts along dimension 0
- output 3: bfloat16 [4, 3200, 1024], P('rep'), parts along dimension 0
- output 4: float32 [4, 1024, 3200], P('rep'), parts along dimension 0
- output 5: float32 [4, 1024, 3200], P('rep'), parts along dimension 0
- output 6: float32 [4, 3200, 1024], P('rep'), parts along dimension 0
- output 7: float32 [4, 1024, 3200], P('rep'), parts along dimension 0
- output 8: float32 [4, 1024, 3200], P('rep'), parts along dimension 0
- output 9: float32 [4, 3200, 1024], P('rep'), parts along dimension 0
There are 2 independent parts. The reference program is written for one: setup_inputs(seed, part) draws one part's arguments, and reference() takes and returns one part's arrays. A program takes and returns all parts, laid end to end along the dimension named above; an argument that names none is the same for every part.
All inputs are finite; a program needn't handle non-finite values.
Results may differ from the reference program's by a relative error of at most 0.022.
Values are sent between devices in bfloat16 or wider.
A program may use at most 1.5 GiB of HBM per device.

```python
import jax
import jax.numpy as jnp
from jax import lax

SEQUENCES = 64
TOKENS = 2048
D = 1024
FF = 3200
LAYERS = 2
NAMES = ("w_gate", "w_up", "w_down")
SHAPES = {"w_gate": (LAYERS, D, FF), "w_up": (LAYERS, D, FF), "w_down": (LAYERS, FF, D)}


def bump(key, n, height):
    away = (jnp.arange(n, dtype=jnp.int32) - jax.random.randint(key, (), 0, n, jnp.int32)) % n
    return jnp.where(away < n // 8, height, 1.0)


def together(key, own, strength):
    shared = jax.random.normal(key, own.shape[1:], jnp.float32)
    return (own + strength * shared) * lax.rsqrt(1 + strength * strength)


def setup_inputs(seed: int = 0, part: int = 0) -> dict:
    kx, kdy, ka, kb, kz, kf, kh, kl, *keys = jax.random.split(jax.random.key(seed), 8 + 3 * len(NAMES))
    kx, kdy, ka, kb = (jax.random.fold_in(k, part) for k in (kx, kdy, ka, kb))
    kw, km, kv = (keys[i::3] for i in range(3))
    shape = (SEQUENCES, TOKENS, D)
    much_x, much_dy = jax.random.uniform(kz, (2,), jnp.float32, 0.0, 1.0)
    loud = 2.0 ** jax.random.uniform(jax.random.fold_in(kz, 1), (), jnp.float32, -1.0, 2.0)
    layers = 2.0 ** jax.random.uniform(kl, (LAYERS, 1, 1), jnp.float32, -1.0, 1.0)
    x = together(ka, jax.random.normal(kx, shape, jnp.float32), much_x) * bump(kf, D, 4.0)
    dy = together(kb, jax.random.normal(kdy, shape, jnp.float32), much_dy)
    drawn = {"x": x.astype(jnp.bfloat16), "dy": (loud * dy * (SEQUENCES * TOKENS) ** -0.5).astype(jnp.bfloat16)}
    for key, name in zip(kw, NAMES, strict=True):
        w = jax.random.normal(key, SHAPES[name], jnp.float32) * SHAPES[name][1] ** -0.5
        drawn[name] = (w * {"w_gate": 1.0, "w_up": bump(kh, FF, 4.0), "w_down": layers}[name]).astype(jnp.bfloat16)
    for key, name in zip(km, NAMES, strict=True):
        drawn[f"m_{name}"] = 0.1 * jax.random.normal(key, SHAPES[name], jnp.float32)
    for key, name in zip(kv, NAMES, strict=True):
        drawn[f"v_{name}"] = loud * loud * jax.random.uniform(key, SHAPES[name], jnp.float32, 0.05, 0.15)
    return drawn


def matmul(a, w):
    return jnp.dot(a, w, preferred_element_type=jnp.float32).astype(jnp.bfloat16)


def normed(h):
    wide = h.astype(jnp.float32)
    scale = lax.rsqrt(jnp.mean(wide**2, -1, keepdims=True) + 1e-6)
    return (wide * scale).astype(jnp.bfloat16)


def layer(h, w):
    a = normed(h)
    gate = jnp.dot(a, w["w_gate"], preferred_element_type=jnp.float32)
    up = jnp.dot(a, w["w_up"], preferred_element_type=jnp.float32)
    return h + matmul((jax.nn.silu(gate) * up).astype(jnp.bfloat16), w["w_down"])


def adamw(w, m, v, g):
    m = 0.9 * m + 0.1 * g
    v = 0.95 * v + 0.05 * g * g
    step = m * lax.rsqrt(v + 1e-8) + 0.1 * w
    return (w - 0.02 * step).astype(jnp.bfloat16), m, v


def stack(weights, h):
    return lax.scan(lambda h, w: (layer(h, w), None), h, weights)[0]


def reference(x, dy, w_gate, w_up, w_down, m_w_gate, m_w_up, m_w_down, v_w_gate, v_w_up, v_w_down):
    weights = dict(zip(NAMES, (w_gate, w_up, w_down), strict=True))

    def take(so_far, sequence):
        h, by_y = sequence
        _, back = jax.vjp(lambda w: stack(w, h), weights)
        return jax.tree.map(lambda total, term: total + term.astype(jnp.float32), so_far, back(by_y)[0]), None

    none_yet = {name: jnp.zeros(w.shape, jnp.float32) for name, w in weights.items()}
    by_weights, _ = lax.scan(take, none_yet, (x, dy))
    gradients = [by_weights[name].astype(jnp.bfloat16).astype(jnp.float32) for name in NAMES]
    new = [
        adamw(w.astype(jnp.float32), m, v, g)
        for w, m, v, g in zip((w_gate, w_up, w_down), (m_w_gate, m_w_up, m_w_down), (v_w_gate, v_w_up, v_w_down), gradients, strict=True)
    ]
    return tuple(one[which] for which in range(3) for one in new)
```

```python
import functools
import jax
import jax.numpy as jnp
from jax import lax
from jax.experimental import pallas as pl
from jax.experimental.pallas import tpu as pltpu
from jax.sharding import PartitionSpec as P

F32, BF = jnp.float32, jnp.bfloat16
TILE = 512

def vmem(mib):
    return pltpu.CompilerParams(vmem_limit_bytes=mib << 20, dimension_semantics=("arbitrary",))

def cost(flops, nbytes):
    return pl.CostEstimate(flops=flops, bytes_accessed=nbytes, transcendentals=0)

def nn(a, b):
    return lax.dot_general(a, b, (((1,), (0,)), ((), ())), preferred_element_type=F32)

def nt(a, b):
    return lax.dot_general(a, b, (((1,), (1,)), ((), ())), preferred_element_type=F32)

def rows(i):
    return pl.ds(i * TILE, TILE)

def sig(x):
    return 1.0 / (1.0 + jnp.exp(-x))

def ready_kernel(x, dy, a, at, dyt):
    wide = x[...].astype(F32)
    n = wide * lax.rsqrt(jnp.mean(wide * wide, -1, keepdims=True) + 1e-6)
    a[...] = n.astype(BF)
    at[...] = n.astype(BF).T
    dyt[...] = dy[...].T

def ready(x, dy, block=256):
    t, d = x.shape
    tok = pl.BlockSpec((block, d), lambda i: (i, 0))
    tokt = pl.BlockSpec((d, block), lambda i: (0, i))
    return pl.pallas_call(
        ready_kernel, grid=(t // block,), in_specs=[tok, tok], out_specs=[tok, tokt, tokt],
        out_shape=[jax.ShapeDtypeStruct((t, d), BF)] + [jax.ShapeDtypeStruct((d, t), BF)] * 2,
        compiler_params=vmem(60), name="ready", cost_estimate=cost(10 * t * d, 10 * t * d),
    )(x, dy)

def gated_kernel(a, wg, wu, act, gate, up):
    for i in range(a.shape[0] // TILE):
        g, u = nn(a[rows(i)], wg[0]), nn(a[rows(i)], wu[0])
        gate[rows(i)] = g
        up[rows(i)] = u
        act[rows(i)] = (g * sig(g) * u).astype(BF)

def gated(a, w_gate, w_up, number, block=256):
    t, d = a.shape
    ff = w_gate.shape[2]
    whole = pl.BlockSpec((t, d), lambda j: (0, 0))
    w = pl.BlockSpec((1, d, block), lambda j: (number, 0, j))
    out = pl.BlockSpec((t, block), lambda j: (0, j))
    return pl.pallas_call(
        gated_kernel, grid=(pl.cdiv(ff, block),), in_specs=[whole, w, w], out_specs=[out] * 3,
        out_shape=[jax.ShapeDtypeStruct((t, ff), x) for x in (BF, F32, F32)],
        compiler_params=vmem(60), name="gated", cost_estimate=cost(4 * t * d * ff, 10 * t * ff + 4 * d * ff),
    )(a, w_gate, w_up)

def down_kernel(act, w, h, out, a, at):
    o = h[...].astype(F32) + nn(act[...], w[0]).astype(BF).astype(F32)
    o = o.astype(BF)
    out[...] = o
    wide = o.astype(F32)
    scale = lax.rsqrt(jnp.mean(wide * wide, -1, keepdims=True) + 1e-6)
    n = wide * scale
    a[...] = n.astype(BF)
    at[...] = n.astype(BF).T

def down(act, w_down, h, number, block=512):
    t, d = h.shape
    ff = act.shape[1]
    tok = pl.BlockSpec((block, d), lambda i: (i, 0))
    return pl.pallas_call(
        down_kernel, grid=(t // block,),
        in_specs=[pl.BlockSpec((block, ff), lambda i: (i, 0)), pl.BlockSpec((1, ff, d), lambda i: (number, 0, 0)), tok],
        out_specs=[tok, tok, pl.BlockSpec((d, block), lambda i: (0, i))],
        out_shape=[jax.ShapeDtypeStruct((t, d), BF)] * 2 + [jax.ShapeDtypeStruct((d, t), BF)],
        compiler_params=vmem(60), name="down", cost_estimate=cost(2 * t * d * ff, 2 * t * ff + 2 * d * ff),
    )(act, w_down, h)

def split(g, u, da):
    s = sig(g)
    silu = g * s
    return (silu * u), da * u * (s + silu * (1.0 - s)), da * silu

LAG = 2
STAGES = 5
STRIDE = (16, 4, 1)


def exchange_scratch(units, block):
    local, kept = 2 * LAG + 1, LAG + 1
    return [
        pltpu.VMEM((3, local, 1152, block), BF),
        pltpu.VMEM((3, units, 2, 256, block), BF),
        pltpu.VMEM((3, units, 2, 128, block), BF),
        pltpu.VMEM((3, local, 256, block), F32),
        pltpu.VMEM((3, kept, 288, block), BF),
        pltpu.VMEM((3, units, 2, 64, block), BF),
        pltpu.VMEM((3, units, 2, 32, block), BF),
        pltpu.VMEM((3, kept, 64, block), F32),
        pltpu.VMEM((3, kept, 64, block), BF),
        pltpu.VMEM((3, units, 3, 16, block), BF),
        pltpu.SemaphoreType.DMA((3, kept, 11)),
        pltpu.SemaphoreType.DMA((3, units, 11)),
    ]


def steps_of(units):
    return units + 1 + STAGES * LAG


def exchange(k, units, out, scratch):
    term, in0, in1, one, one_b, in2, in3, two, two_b, in4, sent, got = scratch
    local, kept = 2 * LAG + 1, LAG + 1
    me = lax.axis_index("dp")
    at = (lax.div(me, 16), lax.rem(lax.div(me, 4), 4), lax.rem(me, 4))

    def near(dim, by):
        return lax.rem(at[dim] + by, 4)

    def peer(dim, by):
        return me + (near(dim, by) - at[dim]) * STRIDE[dim]

    def rows(start, n, step=None):
        return pl.ds(pl.multiple_of(start, step or min(n, 128)), n)

    @pl.when(k == 0)
    def _():
        barrier = pltpu.get_barrier_semaphore()
        for dim in range(3):
            for by in (1, 2, 3):
                pl.semaphore_signal(barrier, inc=1, device_id={"dp": peer(dim, by)}, device_id_type=pl.DeviceIdType.MESH)
        pl.semaphore_wait(barrier, 9)

    def copies(stage, u):
        made = []
        lu, ku = lax.rem(u, local), lax.rem(u, kept)

        def add(c, i, src, dst, dim, by):
            made.append(
                pltpu.make_async_remote_copy(
                    src_ref=src, dst_ref=dst, send_sem=sent.at[c, ku, i], recv_sem=got.at[c, u, i],
                    device_id={"dp": peer(dim, by)}, device_id_type=pl.DeviceIdType.MESH,
                )
            )

        for c in range(3):
            d1, d2, d3 = c, (c + 1) % 3, (c + 2) % 3
            if stage == 0:
                add(c, 0, term.at[c, lu, rows(near(d1, 1) * 256 + 128, 256)], in0.at[c, u, 0], d1, 1)
                add(c, 1, term.at[c, lu, rows(near(d1, 2) * 256 + 128, 256)], in0.at[c, u, 1], d1, 3)
            if stage == 1:
                add(c, 2, in0.at[c, u, 0, pl.ds(128, 128)], in1.at[c, u, 0], d1, 1)
                add(c, 3, in0.at[c, u, 1, pl.ds(0, 128)], in1.at[c, u, 1], d1, 3)
            if stage == 2:
                add(c, 4, one_b.at[c, ku, rows(near(d2, 1) * 64 + 32, 64, 32)], in2.at[c, u, 0], d2, 1)
                add(c, 5, one_b.at[c, ku, rows(near(d2, 2) * 64 + 32, 64, 32)], in2.at[c, u, 1], d2, 3)
            if stage == 3:
                add(c, 6, in2.at[c, u, 0, pl.ds(32, 32)], in3.at[c, u, 0], d2, 1)
                add(c, 7, in2.at[c, u, 1, pl.ds(0, 32)], in3.at[c, u, 1], d2, 3)
            if stage == 4:
                for by in (1, 2, 3):
                    add(c, 7 + by, two_b.at[c, ku, rows(near(d3, by) * 16, 16)], in4.at[c, u, by - 1], d3, by)
        return made

    def wide(ref, c, u, r):
        return ref[c, u, r].astype(F32)

    def work(stage, u):
        lu, ku = lax.rem(u, local), lax.rem(u, kept)
        for c in range(3):
            d1, d2, d3 = c, (c + 1) % 3, (c + 2) % 3
            if stage == 1:
                s = in0[c, u, 0, pl.ds(128, 128)].astype(F32) + wide(term, c, lu, rows(near(d1, 1) * 256, 128))
                in0[c, u, 0, pl.ds(128, 128)] = s.astype(BF)
                s = in0[c, u, 1, pl.ds(0, 128)].astype(F32) + wide(term, c, lu, rows(near(d1, 3) * 256 + 128, 128))
                in0[c, u, 1, pl.ds(0, 128)] = s.astype(BF)
            if stage == 2:
                own = at[d1] * 256
                s = wide(term, c, lu, rows(own, 128)) + in0[c, u, 1, pl.ds(128, 128)].astype(F32) + in1[c, u, 0].astype(F32)
                one[c, lu, pl.ds(0, 128)] = s
                one_b[c, ku, pl.ds(0, 128)] = s.astype(BF)
                one_b[c, ku, pl.ds(256, 32)] = s[:32].astype(BF)
                s = wide(term, c, lu, rows(own + 128, 128)) + in0[c, u, 0, pl.ds(0, 128)].astype(F32) + in1[c, u, 1].astype(F32)
                one[c, lu, pl.ds(128, 128)] = s
                one_b[c, ku, pl.ds(128, 128)] = s.astype(BF)
            if stage == 3:
                s = in2[c, u, 0, pl.ds(32, 32)].astype(F32) + one[c, lu, rows(near(d2, 1) * 64, 32)]
                in2[c, u, 0, pl.ds(32, 32)] = s.astype(BF)
                s = in2[c, u, 1, pl.ds(0, 32)].astype(F32) + one[c, lu, rows(near(d2, 3) * 64 + 32, 32)]
                in2[c, u, 1, pl.ds(0, 32)] = s.astype(BF)
            if stage == 4:
                own = at[d2] * 64
                s = one[c, lu, rows(own, 32)] + in2[c, u, 1, pl.ds(32, 32)].astype(F32) + in3[c, u, 0].astype(F32)
                two[c, ku, pl.ds(0, 32)] = s
                two_b[c, ku, pl.ds(0, 32)] = s.astype(BF)
                s = one[c, lu, rows(own + 32, 32)] + in2[c, u, 0, pl.ds(0, 32)].astype(F32) + in3[c, u, 1].astype(F32)
                two[c, ku, pl.ds(32, 32)] = s
                two_b[c, ku, pl.ds(32, 32)] = s.astype(BF)
            if stage == 5:
                s = two[c, ku, rows(at[d3] * 16, 16)]
                for i in range(3):
                    s = s + in4[c, u, i].astype(F32)
                out[c] = s.astype(BF)

    for stage in range(STAGES + 1):
        u = k - 1 - stage * LAG

        @pl.when((u >= 0) & (u < units))
        def _(stage=stage, u=u):
            if stage:
                for copy in copies(stage - 1, u):
                    copy.wait()
                work(stage, u)
            if stage < STAGES:
                for copy in copies(stage, u):
                    copy.start()


def keep(term, c, slot, i, value):
    term[c, slot, pl.ds(i * TILE, TILE)] = value
    if i == 0:
        term[c, slot, pl.ds(1024, 128)] = value[:128]


def sums(k, units, scratch, pairs):
    for i in range(pairs[0][0].shape[0] // TILE):
        for c, (left, right) in enumerate(pairs):
            keep(scratch[0], c, lax.rem(k, 2 * LAG + 1), i, nn(left[rows(i)], right[...]).astype(BF))


def last_kernel(units, a, at, dy, dyt, wg, wu, wd, out, dg_out, du_out, act, *scratch):
    k = pl.program_id(0)
    exchange(k, units, out, scratch)

    @pl.when(k < units)
    def _():
        for i in range(a.shape[0] // TILE):
            g, u, da = nn(a[rows(i)], wg[0]), nn(a[rows(i)], wu[0]), nt(dy[rows(i)], wd[0]).astype(BF).astype(F32)
            c, dg, du = split(g, u, da)
            act[rows(i)] = c.astype(BF)
            dg_out[rows(i)] = dg.astype(BF)
            du_out[rows(i)] = du.astype(BF)
        sums(k, units, scratch, ((dyt, act), (at, dg_out), (at, du_out)))


def specs(t, d, units, block, number):
    def j(k):
        return jnp.minimum(k, units - 1)

    once = pl.Buffered(1)
    return (
        pl.BlockSpec((t, d), lambda k: (0, 0), pipeline_mode=once),
        pl.BlockSpec((d, t), lambda k: (0, 0), pipeline_mode=once),
        pl.BlockSpec((1, d, block), lambda k: (number, 0, j(k))),
        pl.BlockSpec((1, block, d), lambda k: (number, j(k), 0)),
        pl.BlockSpec((t, block), lambda k: (0, j(k))),
        pl.BlockSpec((3, 16, block), lambda k: (0, 0, jnp.clip(k - 1 - STAGES * LAG, 0, units - 1))),
    )


def sending(number):
    return pltpu.CompilerParams(vmem_limit_bytes=63 << 20, dimension_semantics=("arbitrary",), collective_id=number, has_side_effects=True)


def last(a, at, dy, dyt, w_gate, w_up, w_down, number, block=256):
    t, d = a.shape
    ff = w_gate.shape[2]
    units = pl.cdiv(ff, block)
    tok, tokt, w, wt, hid, out = specs(t, d, units, block, number)
    return pl.pallas_call(
        functools.partial(last_kernel, units), grid=(steps_of(units),),
        in_specs=[tok, tokt, tok, tokt, w, w, wt], out_specs=[out, hid, hid],
        out_shape=[jax.ShapeDtypeStruct((3, 16, ff), BF)] + [jax.ShapeDtypeStruct((t, ff), BF)] * 2,
        scratch_shapes=[pltpu.VMEM((t, block), BF)] + exchange_scratch(units, block),
        compiler_params=sending(1), name="last", cost_estimate=cost(12 * t * d * ff, 4 * t * ff + 12 * d * ff),
    )(a, at, dy, dyt, w_gate, w_up, w_down)


def input_kernel(dg, du, wg, wu, h, dy, out, outt):
    da = (nt(dg[...], wg[0]).astype(BF).astype(F32) + nt(du[...], wu[0]).astype(BF).astype(F32)).astype(BF).astype(F32)
    wide = h[...].astype(F32)
    scale = lax.rsqrt(jnp.mean(wide * wide, -1, keepdims=True) + 1e-6)
    dot = jnp.mean(da * wide, -1, keepdims=True)
    dh = scale * da - wide * (scale * scale * scale * dot)
    o = dy[...].astype(F32) + dh.astype(BF).astype(F32)
    out[...] = o.astype(BF)
    outt[...] = o.astype(BF).T

def inputs(dg, du, w_gate, w_up, h, dy, number, block=512):
    t, d = h.shape
    ff = dg.shape[1]
    tok = pl.BlockSpec((block, d), lambda i: (i, 0))
    hid = pl.BlockSpec((block, ff), lambda i: (i, 0))
    w = pl.BlockSpec((1, d, ff), lambda i: (number, 0, 0), pipeline_mode=pl.Buffered(1))
    return pl.pallas_call(
        input_kernel, grid=(t // block,), in_specs=[hid, hid, w, w, tok, tok],
        out_specs=[tok, pl.BlockSpec((d, block), lambda i: (0, i))],
        out_shape=[jax.ShapeDtypeStruct((t, d), BF), jax.ShapeDtypeStruct((d, t), BF)],
        compiler_params=vmem(60), name="inputs", cost_estimate=cost(4 * t * d * ff, 4 * t * ff + 4 * d * ff),
    )(dg, du, w_gate, w_up, h, dy)

def first_kernel(units, at, dh, dht, wd, gate, up, out, act, dgs, dus, *scratch):
    k = pl.program_id(0)
    exchange(k, units, out, scratch)

    @pl.when(k < units)
    def _():
        for i in range(dh.shape[0] // TILE):
            da = nt(dh[rows(i)], wd[0]).astype(BF).astype(F32)
            c, dg, du = split(gate[rows(i)], up[rows(i)], da)
            act[rows(i)] = c.astype(BF)
            dgs[rows(i)] = dg.astype(BF)
            dus[rows(i)] = du.astype(BF)
        sums(k, units, scratch, ((dht, act), (at, dgs), (at, dus)))


def first(at, dh, dht, w_down, gate, up, number, block=256):
    t, d = dh.shape
    ff = gate.shape[1]
    units = pl.cdiv(ff, block)
    tok, tokt, _, wt, hid, out = specs(t, d, units, block, number)
    return pl.pallas_call(
        functools.partial(first_kernel, units), grid=(steps_of(units),),
        in_specs=[tokt, tok, tokt, wt, hid, hid], out_specs=out,
        out_shape=jax.ShapeDtypeStruct((3, 16, ff), BF),
        scratch_shapes=[pltpu.VMEM((t, block), BF)] * 3 + exchange_scratch(units, block),
        compiler_params=sending(2), name="first", cost_estimate=cost(8 * t * d * ff, 8 * t * ff + 8 * d * ff),
    )(at, dh, dht, w_down, gate, up)


def adamw_kernel(which, g, w, m, v, *refs):
    nw, nm, nv = refs[-3:]

    def part(at, grad):
        m2 = 0.9 * m[0, at] + 0.1 * grad
        v2 = 0.95 * v[0, at] + 0.05 * grad * grad
        wide = w[0, at].astype(F32)
        step = m2 * lax.rsqrt(v2 + 1e-8) + 0.1 * wide
        nw[0, at] = (wide - 0.02 * step).astype(BF)
        nm[0, at] = m2
        nv[0, at] = v2

    if which == 0:
        part(pl.ds(0, w.shape[1]), g[...].reshape(-1, g.shape[-1]).T.astype(F32))
    else:

        @pl.loop(0, 16)
        def _(i):
            a, b = lax.div(i, 4), lax.rem(i, 4)
            part(pl.ds(pl.multiple_of(i * 16, 16), 16), (g[b, 0, a, 0] if which == 1 else g[a, b, 0, 0]).astype(F32))


def adamw(which, g, w, m, v, number, before=None):
    _, r, c = w.shape
    block = 256 if which else 640
    spec = pl.BlockSpec((1, block, c), lambda i: (number, i, 0))
    gs = (
        pl.BlockSpec((4, 4, 4, 1, 16, block), lambda i: (0, 0, 0, 0, 0, i)),
        pl.BlockSpec((4, 1, 4, 1, 16, c), lambda i: (0, i, 0, 1, 0, 0)),
        pl.BlockSpec((4, 4, 1, 1, 16, c), lambda i: (0, 0, i, 2, 0, 0)),
    )[which]
    extra = [] if before is None else list(before)
    return pl.pallas_call(
        functools.partial(adamw_kernel, which), grid=(r // block,),
        in_specs=[gs, spec, spec, spec] + [pl.BlockSpec(memory_space=pl.ANY)] * len(extra),
        out_specs=[spec] * 3,
        out_shape=[jax.ShapeDtypeStruct(w.shape, BF), jax.ShapeDtypeStruct(w.shape, F32), jax.ShapeDtypeStruct(w.shape, F32)],
        input_output_aliases={4 + i: i for i in range(len(extra))},
        compiler_params=vmem(60), name="adamw", cost_estimate=cost(20 * r * c, 22 * r * c),
    )(g, w, m, v, *extra)


def gather(part):
    whole = lax.all_gather(part, "dp", axis=0, tiled=True)
    return whole.reshape(4, 4, 4, 3, 16, -1)


def solution(mesh):
    def step(x, dy, *arrays):
        (w_gate, w_up, w_down), moments, squares = (arrays[i : i + 3] for i in (0, 3, 6))
        x, dy = x[0], dy[0]
        a0, a0t, dyt = ready(x, dy)
        act, gate, up = gated(a0, w_gate, w_up, 0)
        h1, a1, a1t = down(act, w_down, x, 0)
        g1, dg, du = last(a1, a1t, dy, dyt, w_gate, w_up, w_down, 1)
        g1 = gather(g1)
        dh, dht = inputs(dg, du, w_gate, w_up, h1, dy, 1)
        g0 = gather(first(a0t, dh, dht, w_down, gate, up, 0))
        new = [None] * 3
        for number, g in ((1, g1), (0, g0)):
            for which, i in enumerate((2, 0, 1)):
                new[i] = adamw(which, g, arrays[i], moments[i], squares[i], number, new[i])
        return tuple(one[which] for which in range(3) for one in new)

    return jax.shard_map(
        step,
        mesh=mesh,
        in_specs=(P(("rep", "dp"), None, None),) * 2 + (P(None, None, None),) * 9,
        out_specs=(P("rep", None, None),) * 9,
        check_vma=False,
    )
```

```python
import functools
import jax
import jax.numpy as jnp
from jax import lax
from jax.experimental import pallas as pl
from jax.experimental.pallas import tpu as pltpu
from jax.sharding import PartitionSpec as P

F32, BF = jnp.float32, jnp.bfloat16
TILE = 512

def vmem(mib):
    return pltpu.CompilerParams(vmem_limit_bytes=mib << 20, dimension_semantics=("arbitrary",))

def cost(flops, nbytes):
    return pl.CostEstimate(flops=flops, bytes_accessed=nbytes, transcendentals=0)

def nn(a, b):
    return lax.dot_general(a, b, (((1,), (0,)), ((), ())), preferred_element_type=F32)

def nt(a, b):
    return lax.dot_general(a, b, (((1,), (1,)), ((), ())), preferred_element_type=F32)

def rows(i):
    return pl.ds(i * TILE, TILE)

def sig(x):
    return 1.0 / (1.0 + jnp.exp(-x))

def ready_kernel(x, a):
    wide = x[...].astype(F32)
    a[...] = (wide * lax.rsqrt(jnp.mean(wide * wide, -1, keepdims=True) + 1e-6)).astype(BF)


def ready(x, block=512):
    t, d = x.shape
    tok = pl.BlockSpec((block, d), lambda i: (i, 0))
    return pl.pallas_call(
        ready_kernel, grid=(t // block,), in_specs=[tok], out_specs=tok, out_shape=jax.ShapeDtypeStruct((t, d), BF),
        compiler_params=vmem(60), name="ready", cost_estimate=cost(5 * t * d, 4 * t * d),
    )(x)


def gated_kernel(a, wg, wu, dy, act, gate, up, at, dyt):
    n = at.shape[1]
    start = jnp.minimum(pl.program_id(0), a.shape[0] // n - 1) * n
    dyt[...] = dy[...].T
    at[...] = a[pl.ds(pl.multiple_of(start, n), n)].T
    for i in range(a.shape[0] // TILE):
        g, u = nn(a[rows(i)], wg[0]), nn(a[rows(i)], wu[0])
        gate[rows(i)] = g
        up[rows(i)] = u
        act[rows(i)] = (g * sig(g) * u).astype(BF)


def gated(a, dy, w_gate, w_up, number, block=256, tokens=256):
    t, d = a.shape
    ff = w_gate.shape[2]
    whole = pl.BlockSpec((t, d), lambda j: (0, 0), pipeline_mode=pl.Buffered(1))
    w = pl.BlockSpec((1, d, block), lambda j: (number, 0, j))
    out = pl.BlockSpec((t, block), lambda j: (0, j))
    turned = pl.BlockSpec((d, tokens), lambda j: (0, jnp.minimum(j, t // tokens - 1)))
    return pl.pallas_call(
        gated_kernel, grid=(pl.cdiv(ff, block),),
        in_specs=[whole, w, w, pl.BlockSpec((tokens, d), lambda j: (jnp.minimum(j, t // tokens - 1), 0))],
        out_specs=[out] * 3 + [turned] * 2,
        out_shape=[jax.ShapeDtypeStruct((t, ff), x) for x in (BF, F32, F32)] + [jax.ShapeDtypeStruct((d, t), BF)] * 2,
        compiler_params=vmem(60), name="gated", cost_estimate=cost(4 * t * d * ff, 10 * t * ff + 4 * d * ff),
    )(a, w_gate, w_up, dy)


def down_kernel(sub, act, w, h, out, a, at):
    for i in range(act.shape[0] // sub):
        r = pl.ds(i * sub, sub)
        o = (h[r].astype(F32) + nn(act[r], w[0]).astype(BF).astype(F32)).astype(BF)
        out[r] = o
        wide = o.astype(F32)
        n = (wide * lax.rsqrt(jnp.mean(wide * wide, -1, keepdims=True) + 1e-6)).astype(BF)
        a[r] = n
        at[:, r] = n.T


def down(act, w_down, h, number, block=512, sub=256):
    t, d = h.shape
    ff = act.shape[1]
    tok = pl.BlockSpec((block, d), lambda i: (i, 0))
    return pl.pallas_call(
        functools.partial(down_kernel, sub), grid=(t // block,),
        in_specs=[pl.BlockSpec((block, ff), lambda i: (i, 0)), pl.BlockSpec((1, ff, d), lambda i: (number, 0, 0), pipeline_mode=pl.Buffered(1)), tok],
        out_specs=[tok, tok, pl.BlockSpec((d, block), lambda i: (0, i))],
        out_shape=[jax.ShapeDtypeStruct((t, d), BF)] * 2 + [jax.ShapeDtypeStruct((d, t), BF)],
        compiler_params=vmem(60), name="down", cost_estimate=cost(2 * t * d * ff, 2 * t * ff + 2 * d * ff),
    )(act, w_down, h)

def split(g, u, da):
    s = sig(g)
    silu = g * s
    return (silu * u), da * u * (s + silu * (1.0 - s)), da * silu

STAGES = 5
STRIDE = (16, 4, 1)


def exchange_scratch(units, block, lag):
    local, kept = 2 * lag + 1, lag + 1
    return [
        pltpu.VMEM((3, local, 1152, block), BF),
        pltpu.VMEM((3, units, 2, 256, block), BF),
        pltpu.VMEM((3, units, 2, 128, block), BF),
        pltpu.VMEM((3, local, 256, block), F32),
        pltpu.VMEM((3, kept, 288, block), BF),
        pltpu.VMEM((3, units, 2, 64, block), BF),
        pltpu.VMEM((3, units, 2, 32, block), BF),
        pltpu.VMEM((3, kept, 64, block), F32),
        pltpu.VMEM((3, kept, 64, block), BF),
        pltpu.VMEM((3, units, 3, 16, block), BF),
        pltpu.SemaphoreType.DMA((3, kept, 11)),
        pltpu.SemaphoreType.DMA((3, units, 11)),
    ]


def steps_of(units, lag):
    return units + 1 + STAGES * lag


def exchange(k, units, lag, out, scratch):
    term, in0, in1, one, one_b, in2, in3, two, two_b, in4, sent, got = scratch
    local, kept = 2 * lag + 1, lag + 1
    me = lax.axis_index("dp")
    at = (lax.div(me, 16), lax.rem(lax.div(me, 4), 4), lax.rem(me, 4))

    def near(dim, by):
        return lax.rem(at[dim] + by, 4)

    def peer(dim, by):
        return me + (near(dim, by) - at[dim]) * STRIDE[dim]

    def rows(start, n, step=None):
        return pl.ds(pl.multiple_of(start, step or min(n, 128)), n)

    @pl.when(k == 0)
    def _():
        barrier = pltpu.get_barrier_semaphore()
        for dim in range(3):
            for by in (1, 2, 3):
                pl.semaphore_signal(barrier, inc=1, device_id={"dp": peer(dim, by)}, device_id_type=pl.DeviceIdType.MESH)
        pl.semaphore_wait(barrier, 9)

    def copies(stage, u):
        made = []
        lu, ku = lax.rem(u, local), lax.rem(u, kept)

        def add(c, i, src, dst, dim, by):
            made.append(
                pltpu.make_async_remote_copy(
                    src_ref=src, dst_ref=dst, send_sem=sent.at[c, ku, i], recv_sem=got.at[c, u, i],
                    device_id={"dp": peer(dim, by)}, device_id_type=pl.DeviceIdType.MESH,
                )
            )

        for c in range(3):
            d1, d2, d3 = c, (c + 1) % 3, (c + 2) % 3
            if stage == 0:
                add(c, 0, term.at[c, lu, rows(near(d1, 1) * 256 + 128, 256)], in0.at[c, u, 0], d1, 1)
                add(c, 1, term.at[c, lu, rows(near(d1, 2) * 256 + 128, 256)], in0.at[c, u, 1], d1, 3)
            if stage == 1:
                add(c, 2, in0.at[c, u, 0, pl.ds(128, 128)], in1.at[c, u, 0], d1, 1)
                add(c, 3, in0.at[c, u, 1, pl.ds(0, 128)], in1.at[c, u, 1], d1, 3)
            if stage == 2:
                add(c, 4, one_b.at[c, ku, rows(near(d2, 1) * 64 + 32, 64, 32)], in2.at[c, u, 0], d2, 1)
                add(c, 5, one_b.at[c, ku, rows(near(d2, 2) * 64 + 32, 64, 32)], in2.at[c, u, 1], d2, 3)
            if stage == 3:
                add(c, 6, in2.at[c, u, 0, pl.ds(32, 32)], in3.at[c, u, 0], d2, 1)
                add(c, 7, in2.at[c, u, 1, pl.ds(0, 32)], in3.at[c, u, 1], d2, 3)
            if stage == 4:
                for by in (1, 2, 3):
                    add(c, 7 + by, two_b.at[c, ku, rows(near(d3, by) * 16, 16)], in4.at[c, u, by - 1], d3, by)
        return made

    def wide(ref, c, u, r):
        return ref[c, u, r].astype(F32)

    def work(stage, u):
        lu, ku = lax.rem(u, local), lax.rem(u, kept)
        for c in range(3):
            d1, d2, d3 = c, (c + 1) % 3, (c + 2) % 3
            if stage == 1:
                s = in0[c, u, 0, pl.ds(128, 128)].astype(F32) + wide(term, c, lu, rows(near(d1, 1) * 256, 128))
                in0[c, u, 0, pl.ds(128, 128)] = s.astype(BF)
                s = in0[c, u, 1, pl.ds(0, 128)].astype(F32) + wide(term, c, lu, rows(near(d1, 3) * 256 + 128, 128))
                in0[c, u, 1, pl.ds(0, 128)] = s.astype(BF)
            if stage == 2:
                own = at[d1] * 256
                s = wide(term, c, lu, rows(own, 128)) + in0[c, u, 1, pl.ds(128, 128)].astype(F32) + in1[c, u, 0].astype(F32)
                one[c, lu, pl.ds(0, 128)] = s
                one_b[c, ku, pl.ds(0, 128)] = s.astype(BF)
                one_b[c, ku, pl.ds(256, 32)] = s[:32].astype(BF)
                s = wide(term, c, lu, rows(own + 128, 128)) + in0[c, u, 0, pl.ds(0, 128)].astype(F32) + in1[c, u, 1].astype(F32)
                one[c, lu, pl.ds(128, 128)] = s
                one_b[c, ku, pl.ds(128, 128)] = s.astype(BF)
            if stage == 3:
                s = in2[c, u, 0, pl.ds(32, 32)].astype(F32) + one[c, lu, rows(near(d2, 1) * 64, 32)]
                in2[c, u, 0, pl.ds(32, 32)] = s.astype(BF)
                s = in2[c, u, 1, pl.ds(0, 32)].astype(F32) + one[c, lu, rows(near(d2, 3) * 64 + 32, 32)]
                in2[c, u, 1, pl.ds(0, 32)] = s.astype(BF)
            if stage == 4:
                own = at[d2] * 64
                s = one[c, lu, rows(own, 32)] + in2[c, u, 1, pl.ds(32, 32)].astype(F32) + in3[c, u, 0].astype(F32)
                two[c, ku, pl.ds(0, 32)] = s
                two_b[c, ku, pl.ds(0, 32)] = s.astype(BF)
                s = one[c, lu, rows(own + 32, 32)] + in2[c, u, 0, pl.ds(0, 32)].astype(F32) + in3[c, u, 1].astype(F32)
                two[c, ku, pl.ds(32, 32)] = s
                two_b[c, ku, pl.ds(32, 32)] = s.astype(BF)
            if stage == 5:
                s = two[c, ku, rows(at[d3] * 16, 16)]
                for i in range(3):
                    s = s + in4[c, u, i].astype(F32)
                out[c] = s.astype(BF)

    for stage in range(STAGES + 1):
        u = k - 1 - stage * lag

        @pl.when((u >= 0) & (u < units))
        def _(stage=stage, u=u):
            if stage:
                for copy in copies(stage - 1, u):
                    copy.wait()
                work(stage, u)
            if stage < STAGES:
                for copy in copies(stage, u):
                    copy.start()


def keep(term, c, slot, i, value):
    term[c, slot, pl.ds(i * TILE, TILE)] = value
    if i == 0:
        term[c, slot, pl.ds(1024, 128)] = value[:128]


def sums(k, lag, scratch, pairs):
    for i in range(pairs[0][0].shape[0] // TILE):
        for c, (left, right) in enumerate(pairs):
            keep(scratch[0], c, lax.rem(k, 2 * lag + 1), i, nn(left[rows(i)], right[...]).astype(BF))


def last_kernel(units, lag, a, at, dy, dyt, wg, wu, wd, out, dg_out, du_out, act, *scratch):
    k = pl.program_id(0)
    exchange(k, units, lag, out, scratch)

    @pl.when(k < units)
    def _():
        for i in range(a.shape[0] // TILE):
            g, u, da = nn(a[rows(i)], wg[0]), nn(a[rows(i)], wu[0]), nt(dy[rows(i)], wd[0]).astype(BF).astype(F32)
            c, dg, du = split(g, u, da)
            act[rows(i)] = c.astype(BF)
            dg_out[rows(i)] = dg.astype(BF)
            du_out[rows(i)] = du.astype(BF)
        sums(k, lag, scratch, ((dyt, act), (at, dg_out), (at, du_out)))


def specs(t, d, units, lag, block, number):
    def j(k):
        return jnp.minimum(k, units - 1)

    once = pl.Buffered(1)
    return (
        pl.BlockSpec((t, d), lambda k: (0, 0), pipeline_mode=once),
        pl.BlockSpec((d, t), lambda k: (0, 0), pipeline_mode=once),
        pl.BlockSpec((1, d, block), lambda k: (number, 0, j(k))),
        pl.BlockSpec((1, block, d), lambda k: (number, j(k), 0)),
        pl.BlockSpec((t, block), lambda k: (0, j(k))),
        pl.BlockSpec((3, 16, block), lambda k: (0, 0, jnp.clip(k - 1 - STAGES * lag, 0, units - 1))),
    )


def sending(number):
    return pltpu.CompilerParams(vmem_limit_bytes=63 << 20, dimension_semantics=("arbitrary",), collective_id=number, has_side_effects=True)


def last(a, at, dy, dyt, w_gate, w_up, w_down, number, block=256, lag=1):
    t, d = a.shape
    ff = w_gate.shape[2]
    units = pl.cdiv(ff, block)
    tok, tokt, w, wt, hid, out = specs(t, d, units, lag, block, number)
    return pl.pallas_call(
        functools.partial(last_kernel, units, lag), grid=(steps_of(units, lag),),
        in_specs=[tok, tokt, tok, tokt, w, w, wt], out_specs=[out, hid, hid],
        out_shape=[jax.ShapeDtypeStruct((3, 16, ff), BF)] + [jax.ShapeDtypeStruct((t, ff), BF)] * 2,
        scratch_shapes=[pltpu.VMEM((t, block), BF)] + exchange_scratch(units, block, lag),
        compiler_params=sending(1), name="last", cost_estimate=cost(12 * t * d * ff, 4 * t * ff + 12 * d * ff),
    )(a, at, dy, dyt, w_gate, w_up, w_down)


def input_kernel(sub, dg, du, wg, wu, h, dy, out, outt):
    for i in range(dg.shape[0] // sub):
        r = pl.ds(i * sub, sub)
        da = (nt(dg[r], wg[0]).astype(BF).astype(F32) + nt(du[r], wu[0]).astype(BF).astype(F32)).astype(BF).astype(F32)
        wide = h[r].astype(F32)
        scale = lax.rsqrt(jnp.mean(wide * wide, -1, keepdims=True) + 1e-6)
        dot = jnp.mean(da * wide, -1, keepdims=True)
        dh = scale * da - wide * (scale * scale * scale * dot)
        o = (dy[r].astype(F32) + dh.astype(BF).astype(F32)).astype(BF)
        out[r] = o
        outt[:, r] = o.T


def inputs(dg, du, w_gate, w_up, h, dy, number, block=512, sub=256):
    t, d = h.shape
    ff = dg.shape[1]
    tok = pl.BlockSpec((block, d), lambda i: (i, 0))
    hid = pl.BlockSpec((block, ff), lambda i: (i, 0))
    w = pl.BlockSpec((1, d, ff), lambda i: (number, 0, 0), pipeline_mode=pl.Buffered(1))
    return pl.pallas_call(
        functools.partial(input_kernel, sub), grid=(t // block,), in_specs=[hid, hid, w, w, tok, tok],
        out_specs=[tok, pl.BlockSpec((d, block), lambda i: (0, i))],
        out_shape=[jax.ShapeDtypeStruct((t, d), BF), jax.ShapeDtypeStruct((d, t), BF)],
        compiler_params=vmem(60), name="inputs", cost_estimate=cost(4 * t * d * ff, 4 * t * ff + 4 * d * ff),
    )(dg, du, w_gate, w_up, h, dy)

def first_kernel(units, lag, at, dh, dht, wd, gate, up, out, act, dgs, dus, *scratch):
    k = pl.program_id(0)
    exchange(k, units, lag, out, scratch)

    @pl.when(k < units)
    def _():
        for i in range(dh.shape[0] // TILE):
            da = nt(dh[rows(i)], wd[0]).astype(BF).astype(F32)
            c, dg, du = split(gate[rows(i)], up[rows(i)], da)
            act[rows(i)] = c.astype(BF)
            dgs[rows(i)] = dg.astype(BF)
            dus[rows(i)] = du.astype(BF)
        sums(k, lag, scratch, ((dht, act), (at, dgs), (at, dus)))


def first(at, dh, dht, w_down, gate, up, number, block=256, lag=2):
    t, d = dh.shape
    ff = gate.shape[1]
    units = pl.cdiv(ff, block)
    tok, tokt, _, wt, hid, out = specs(t, d, units, lag, block, number)
    return pl.pallas_call(
        functools.partial(first_kernel, units, lag), grid=(steps_of(units, lag),),
        in_specs=[tokt, tok, tokt, wt, hid, hid], out_specs=out,
        out_shape=jax.ShapeDtypeStruct((3, 16, ff), BF),
        scratch_shapes=[pltpu.VMEM((t, block), BF)] * 3 + exchange_scratch(units, block, lag),
        compiler_params=sending(2), name="first", cost_estimate=cost(8 * t * d * ff, 8 * t * ff + 8 * d * ff),
    )(at, dh, dht, w_down, gate, up)


def adamw_kernel(which, g, w, m, v, *refs):
    nw, nm, nv = refs[-3:]

    def part(at, grad):
        m2 = 0.9 * m[0, at] + 0.1 * grad
        v2 = 0.95 * v[0, at] + 0.05 * grad * grad
        wide = w[0, at].astype(F32)
        step = m2 * lax.rsqrt(v2 + 1e-8) + 0.1 * wide
        nw[0, at] = (wide - 0.02 * step).astype(BF)
        nm[0, at] = m2
        nv[0, at] = v2

    if which == 0:
        part(pl.ds(0, w.shape[1]), g[...].reshape(-1, g.shape[-1]).T.astype(F32))
    else:

        @pl.loop(0, 16)
        def _(i):
            a, b = lax.div(i, 4), lax.rem(i, 4)
            part(pl.ds(pl.multiple_of(i * 16, 16), 16), (g[b, 0, a, 0] if which == 1 else g[a, b, 0, 0]).astype(F32))


def adamw(which, g, w, m, v, number, before=None):
    _, r, c = w.shape
    block = 256 if which else 640
    spec = pl.BlockSpec((1, block, c), lambda i: (number, i, 0))
    gs = (
        pl.BlockSpec((4, 4, 4, 1, 16, block), lambda i: (0, 0, 0, 0, 0, i)),
        pl.BlockSpec((4, 1, 4, 1, 16, c), lambda i: (0, i, 0, 1, 0, 0)),
        pl.BlockSpec((4, 4, 1, 1, 16, c), lambda i: (0, 0, i, 2, 0, 0)),
    )[which]
    extra = [] if before is None else list(before)
    return pl.pallas_call(
        functools.partial(adamw_kernel, which), grid=(r // block,),
        in_specs=[gs, spec, spec, spec] + [pl.BlockSpec(memory_space=pl.ANY)] * len(extra),
        out_specs=[spec] * 3,
        out_shape=[jax.ShapeDtypeStruct(w.shape, BF), jax.ShapeDtypeStruct(w.shape, F32), jax.ShapeDtypeStruct(w.shape, F32)],
        input_output_aliases={4 + i: i for i in range(len(extra))},
        compiler_params=vmem(60), name="adamw", cost_estimate=cost(20 * r * c, 22 * r * c),
    )(g, w, m, v, *extra)


def gather(part):
    whole = lax.all_gather(part, "dp", axis=0, tiled=True)
    return whole.reshape(4, 4, 4, 3, 16, -1)


def solution(mesh):
    def step(x, dy, *arrays):
        (w_gate, w_up, w_down), moments, squares = (arrays[i : i + 3] for i in (0, 3, 6))
        x, dy = x[0], dy[0]
        act, gate, up, a0t, dyt = gated(ready(x), dy, w_gate, w_up, 0)
        h1, a1, a1t = down(act, w_down, x, 0)
        g1, dg, du = last(a1, a1t, dy, dyt, w_gate, w_up, w_down, 1)
        g1 = gather(g1)
        dh, dht = inputs(dg, du, w_gate, w_up, h1, dy, 1)
        g0 = gather(first(a0t, dh, dht, w_down, gate, up, 0))
        new = [None] * 3
        for number, g in ((1, g1), (0, g0)):
            for which, i in enumerate((2, 0, 1)):
                new[i] = adamw(which, g, arrays[i], moments[i], squares[i], number, new[i])
        return tuple(one[which] for which in range(3) for one in new)

    return jax.shard_map(
        step,
        mesh=mesh,
        in_specs=(P(("rep", "dp"), None, None),) * 2 + (P(None, None, None),) * 9,
        out_specs=(P("rep", None, None),) * 9,
        check_vma=False,
    )
```
